32 devices in a mesh: gx: 2 (over x), gy: 4 (over y, core), gz: 4 (over z).
Axes of the slice: x: 2, y: 2, z: 4, core: 2. Of those that a mesh axis runs over, the one named last changes fastest.
Arguments:
- rhs: float32 [8, 8, 2, 16, 512], P(None, None, 'gx', 'gy', 'gz'), as said below
- blocks: bfloat16 [7, 8, 8, 2, 16, 512], P(None, None, None, 'gx', 'gy', 'gz'), as said below
Outputs:
- basis: float32 [4, 8, 8, 2, 16, 512], P(None, None, None, 'gx', 'gy', 'gz')
- hess: float32 [4, 8, 3, 8], replicated
Inputs may be any that keep to these rules, and one draw needn't show every extreme that they name: `rhs`: each cell's value is a random draw times a positive scale that varies smoothly over the grid. The operator couples each cell only to itself and its six face neighbours; its blocks are full and the block Krylov spaces keep full rank.
All inputs are finite; a program needn't handle non-finite values.
Results may differ from the reference program's by a relative error of at most 0.001.
Values sent between devices are 32-bit elements; how exact they have to be, the bound alone decides.
A program may use at most 64 MiB of HBM per device.

```python
import jax
import jax.numpy as jnp
from jax import lax

BLOCK = 8
RHS = 8
ITERS = 3
NX = 2
NY = 16
NZ = 512


def draw_rhs(key, part):
    shape = (BLOCK, RHS, NX, NY, NZ)
    values = jax.random.normal(key, shape, jnp.float32)
    pos_x = jnp.arange(NX, dtype=jnp.float32)[:, None, None] / NX
    pos_y = jnp.arange(NY, dtype=jnp.float32)[None, :, None] / NY
    pos_z = jnp.arange(NZ, dtype=jnp.float32)[None, None, :] / NZ
    rising = 3.0 ** pos_z * 2.0 ** pos_x * 2.0 ** pos_y
    return values * rising[None, None]


def draw_blocks(key, part):
    key_noise = jax.random.fold_in(key, 11)
    key_center = jax.random.fold_in(key, 12)
    key_flow = jax.random.fold_in(key, 13)
    shape = (7, BLOCK, BLOCK, NX, NY, NZ)
    noise = jax.random.normal(key_noise, shape, jnp.float32)
    center = jax.random.uniform(key_center, (NX, NY, NZ), jnp.float32, 0.0, 1.0)
    flow = jax.random.uniform(key_flow, (3, NX, NY, NZ), jnp.float32, -1.0, 1.0)
    eye = jnp.eye(BLOCK, dtype=jnp.float32)[:, :, None, None, None]
    parts = [(0.8 + 0.4 * center)[None, None] * eye + 0.06 * noise[0]]
    for k in range(1, 7):
        axis_number = (k - 1) // 2
        sign = 1.0 if k % 2 == 1 else -1.0
        weight = -(0.125 + 0.06 * sign * flow[axis_number])
        parts.append(weight[None, None] * eye + 0.02 * noise[k])
    return jnp.stack(parts).astype(jnp.bfloat16)


def setup_inputs(seed: int = 0) -> dict:
    arg_keys = jax.random.split(jax.random.key(seed), 3)
    rhs = draw_rhs(jax.random.fold_in(arg_keys[2], 71), 0)
    blocks = draw_blocks(jax.random.fold_in(arg_keys[2], 71), 0)
    return {"rhs": rhs, "blocks": blocks}


HIGH = lax.Precision.HIGHEST

def operate(field, blocks):
    padded = jnp.pad(field, ((0, 0), (0, 0), (1, 1), (1, 1), (1, 1)))
    views = [padded[:, :, 1:-1, 1:-1, 1:-1], padded[:, :, 2:, 1:-1, 1:-1], padded[:, :, :-2, 1:-1, 1:-1], padded[:, :, 1:-1, 2:, 1:-1], padded[:, :, 1:-1, :-2, 1:-1], padded[:, :, 1:-1, 1:-1, 2:], padded[:, :, 1:-1, 1:-1, :-2]]
    total = jnp.zeros(field.shape, jnp.float32)
    for k in range(7):
        for j in range(field.shape[0]):
            column = blocks[k, :, j].astype(jnp.float32)
            total = total + column[:, None] * views[k][j][None]
    return total

def pair(first, second):
    return jnp.einsum('arxyz,asxyz->rs', first, second, precision=HIGH)

def mix(field, matrix):
    return jnp.einsum('asxyz,sr->arxyz', field, matrix, precision=HIGH)

def normalizer(gram, eye):
    lower = jnp.linalg.cholesky(gram)
    inverse = lax.linalg.triangular_solve(lower, eye, left_side=True, lower=True)
    return (inverse.T, lower.T)

def reference(rhs, blocks):
    eye = jnp.eye(RHS, dtype=jnp.float32)
    scale, upper = normalizer(pair(rhs, rhs), eye)
    basis = [mix(rhs, scale)]
    hess = jnp.zeros((ITERS + 1, RHS, ITERS, RHS), jnp.float32)
    for step in range(ITERS):
        image = operate(basis[step], blocks)
        coeffs = [pair(vector, image) for vector in basis]
        gram = pair(image, image)
        rest = image
        for vector, coeff in zip(basis, coeffs):
            gram = gram - jnp.dot(coeff.T, coeff, precision=HIGH)
            rest = rest - mix(vector, coeff)
        scale, upper = normalizer(gram, eye)
        basis.append(mix(rest, scale))
        for index, coeff in enumerate(coeffs):
            hess = hess.at[index, :, step, :].set(coeff)
        hess = hess.at[step + 1, :, step, :].set(upper)
    return (jnp.stack(basis), hess)
```

```python
import functools

import jax
import jax.numpy as jnp
from jax import lax
from jax.experimental import pallas as pl
from jax.experimental.pallas import tpu as pltpu
from jax.sharding import PartitionSpec as P

ITERS = 3
F32 = jnp.float32
HIGH = lax.Precision.HIGHEST
AXES = ("gx", "gy", "gz")


def dot_nt(a, b):
    return lax.dot_general(a, b, (((1,), (1,)), ((), ())), precision=HIGH, preferred_element_type=F32)


def dot_nn(a, b):
    return lax.dot_general(a, b, (((1,), (0,)), ((), ())), precision=HIGH, preferred_element_type=F32)


def kernel(
    mesh_sizes, nb, nr, ly, lz,
    rhs_hbm, blk_hbm, basis_hbm, hess_ref,
    rv, bv, vp, p1, p3, xb, zs, zr, ce, zp, ab, ob,
    x_send, x_recv, y_send, y_recv, z_send, z_recv, a_send, a_recv, in_sem, out_sem,
):
    nx, ny, nz = mesh_sizes
    ndev = nx * ny * nz
    gx, gy, gz = (lax.axis_index(a) for a in AXES)
    me = (gx * ny + gy) * nz + gz
    cells = ndev * ly * lz

    row = lax.broadcasted_iota(jnp.int32, (8, 128), 0)
    lane = lax.broadcasted_iota(jnp.int32, (8, 128), 1)

    in_rhs = pltpu.make_async_copy(rhs_hbm, rv, in_sem.at[0])
    in_blk = pltpu.make_async_copy(blk_hbm, bv, in_sem.at[1])
    in_rhs.start()
    in_blk.start()

    if nx == 1:
        x_sides = []
    elif nx == 2:
        x_sides = [(1 + gx, None, 1 - gx)]
    else:
        x_sides = [(1, gx < nx - 1, gx + 1), (2, gx > 0, gx - 1)]

    def when(cond, fn):
        if cond is None:
            fn()
        else:
            pl.when(cond)(fn)

    def remote(src, dst, ssem, rsem, dev):
        return pltpu.make_async_remote_copy(
            src_ref=src, dst_ref=dst, send_sem=ssem, recv_sem=rsem,
            device_id=dev, device_id_type=pl.DeviceIdType.MESH,
        )

    def x_copy(n, side, y):
        opposite = side if nx == 2 else 1 - side
        return remote(vp.at[n, 1 + y], xb.at[n, opposite, y], x_send.at[n, side, y],
                      x_recv.at[n, opposite, y], {"gx": x_sides[side][2]})

    def x_arrived(n, side, y):
        remote(vp.at[n, 1 + y], xb.at[n, side, y], x_send.at[n, side, y],
               x_recv.at[n, side, y], {"gx": x_sides[side][2]}).wait_recv()

    def y_copy(n, side):
        if side == 0:
            return remote(vp.at[n, ly], vp.at[n, 0], y_send.at[n, 0], y_recv.at[n, 0], {"gy": gy + 1})
        return remote(vp.at[n, 1], vp.at[n, ly + 1], y_send.at[n, 1], y_recv.at[n, 1], {"gy": gy - 1})

    def z_copy(n, side, y):
        target = gz - 1 if side == 0 else gz + 1
        return remote(zs.at[n, side, y], zr.at[n, side, y], z_send.at[n, side, y],
                      z_recv.at[n, side, y], {"gz": target})

    y_to = (gy < ny - 1, gy > 0)
    y_from = (gy > 0, gy < ny - 1)
    z_to = (gz > 0, gz < nz - 1)
    z_from = (gz < nz - 1, gz > 0)

    for side in range(2):
        @pl.when(jnp.logical_not(y_from[side]))
        def _():
            for n in range(ITERS):
                vp[n, 0 if side == 0 else ly + 1] = jnp.zeros((nb * 8, 128), F32)

        @pl.when(jnp.logical_not(z_from[side]))
        def _():
            for n in range(ITERS):
                zr[n, side] = jnp.zeros((ly, 8, 128), F32)

    if nx > 2:
        for side in range(2):
            @pl.when(jnp.logical_not(x_sides[side][1]))
            def _():
                for n in range(ITERS):
                    xb[n, side] = jnp.zeros((ly, nb * 8, 128), F32)

    def send_row(n, y):
        for side, entry in enumerate(x_sides):
            when(entry[1], lambda: x_copy(n, side, y).start())
        first = jnp.zeros((8, 128), F32)
        last = jnp.zeros((8, 128), F32)
        for a in range(nb):
            v = vp[n, 1 + y, a * 8:(a + 1) * 8]
            first = jnp.where(lane == a, pltpu.roll(v, a, 1) if a else v, first)
            last = jnp.where(lane == a, pltpu.roll(v, a + 1, 1), last)
        zs[n, 0, y] = first
        zs[n, 1, y] = last
        for side in range(2):
            pl.when(z_to[side])(lambda: z_copy(n, side, y).start())
        if y == ly - 1:
            pl.when(y_to[0])(lambda: y_copy(n, 0).start())
        if y == 0:
            pl.when(y_to[1])(lambda: y_copy(n, 1).start())

    order = [0] + ([ly - 1] if ly > 1 else []) + list(range(1, ly - 1))

    in_rhs.wait()
    for y in order:
        for a in range(nb):
            vp[0, 1 + y, a * 8:(a + 1) * 8] = rv[pl.ds(a * nr * ly + y, 8, stride=ly), :]
        send_row(0, y)

    in_blk.wait()
    terms = [0, 3, 4, 5, 6] + [e[0] for e in x_sides]
    total_abs = jnp.zeros((8, 128), F32)
    for t, k in enumerate(terms):
        def expand(i, carry):
            rows = bv[k, i].astype(F32)
            for j in range(nb):
                for y in range(ly):
                    r = j * ly + y
                    wide = jnp.broadcast_to(rows[r:r + 1], (8, 128))
                    ce[t, y, j, pl.ds(pl.multiple_of(i * 8, 8), 8), :] = wide
                    if j == 0 and y == 0:
                        pass
            return carry + jnp.sum(jnp.abs(rows), axis=0, keepdims=True)
        total_abs = lax.fori_loop(0, nb, expand, total_abs)
    trace = jnp.zeros((8, 128), F32)
    for y in range(ly):
        for i in range(nb):
            trace = trace + ce[0, y, i, i * 8:(i + 1) * 8]

    def wide(field):
        return jnp.concatenate(
            [field(y, a) for y in range(ly) for a in range(nb)], axis=1)

    def blockview(ref, n, off):
        if n is None:
            return lambda y, a: ref[y, a * 8:(a + 1) * 8]
        return lambda y, a: ref[n, off + y, a * 8:(a + 1) * 8]

    views = [blockview(vp, 0, 1), blockview(p1, None, 0), blockview(vp, 2, 1), blockview(p3, None, 0)]

    def stack(count):
        return jnp.concatenate([wide(v) for v in views[:count]], axis=0)

    def gram(n):
        d = dot_nt(wide(views[n]), stack(n + 1))
        w = 8 * (n + 1)
        rep_l = lax.broadcasted_iota(jnp.int32, (w, 128), 0)
        rep_m = lax.broadcasted_iota(jnp.int32, (w, 128), 1)
        return dot_nn(d, jnp.where(rep_m % 32 == rep_l, 1.0, 0.0).astype(F32))

    def peer(d):
        t = lax.rem(me + d, ndev)
        return (t // (ny * nz), (t // nz) % ny, t % nz)

    def ar_start(m, d8):
        packed = jnp.where(lane // 32 == row % 4, d8, 0.0)
        ab[m, me, 0:1] = jnp.sum(packed[0:4], axis=0, keepdims=True)
        ab[m, me, 1:2] = jnp.sum(packed[4:8], axis=0, keepdims=True)

        def body(d, c):
            remote(ab.at[m, me], ab.at[m, me], a_send.at[m], a_recv.at[m], peer(d)).start()
            return c
        lax.fori_loop(1, ndev, body, 0)

    def ar_done(m):
        pltpu.make_async_copy(ab.at[m, 0:ndev - 1], ab.at[m, 0:ndev - 1], a_recv.at[m]).wait()
        total = jnp.sum(ab[m], axis=0)
        z = jnp.where(row < 4, total[0:1], total[1:2])
        z = jnp.where(lane // 32 == row % 4, z, 0.0)
        z = z + pltpu.roll(z, 64, 1)
        return z + pltpu.roll(z, 32, 1)

    lane_sum = lambda x: jnp.sum(x, axis=1, keepdims=True)
    d0 = gram(0)
    d0 = d0 + jnp.where(lane % 32 == 8, lane_sum(trace), 0.0)
    d0 = d0 + jnp.where(lane % 32 == 9, lane_sum(total_abs), 0.0)
    ar_start(0, d0)

    def local_terms(n, y):
        pl_z = [z_from[0], z_from[1]]
        for side in range(2):
            pl.when(pl_z[side])(lambda: z_copy(n, side, y).wait_recv())
        if y == 0:
            pl.when(y_from[0])(lambda: y_copy(n, 0).wait_recv())
        if y == ly - 1:
            pl.when(y_from[1])(lambda: y_copy(n, 1).wait_recv())
        plus, minus = zr[n, 0, y], zr[n, 1, y]
        for j in range(nb):
            v = vp[n, 1 + y, j * 8:(j + 1) * 8]
            zp[0, j * 8:(j + 1) * 8] = jnp.where(
                lane == lz - 1, pltpu.roll(plus, lz - 1 - j, 1), pltpu.roll(v, lz - 1, 1))
            zp[1, j * 8:(j + 1) * 8] = jnp.where(
                lane == 0, pltpu.roll(minus, lz - j, 1) if j else minus, pltpu.roll(v, 1, 1))

        def body(j, acc):
            at = pl.ds(pl.multiple_of(j * 8, 8), 8)
            values = [vp[n, 1 + y, at, :], vp[n, 2 + y, at, :], vp[n, y, at, :], zp[0, at, :], zp[1, at, :]]
            for t, v in enumerate(values):
                acc = acc + ce[t, y, j].reshape(nb, 8, 128) * v[None]
            return acc
        return lax.fori_loop(0, nb, body, jnp.zeros((nb, 8, 128), F32))

    def x_terms(n, y, acc):
        for side, entry in enumerate(x_sides):
            when(entry[1], lambda: x_arrived(n, side, y))

            def body(j, acc):
                at = pl.ds(pl.multiple_of(j * 8, 8), 8)
                return acc + ce[5 + side, y, j].reshape(nb, 8, 128) * xb[n, side, y, at, :][None]
            acc = lax.fori_loop(0, nb, body, acc)
        return acc.reshape(nb * 8, 128)

    for y in order:
        vp[1, 1 + y] = x_terms(0, y, local_terms(0, y))
        send_row(1, y)
    red0 = ar_done(0)
    sigma = jnp.broadcast_to(red0[0:1, 8:9] / (8.0 * cells), (8, 128))
    nu = jnp.broadcast_to(red0[0:1, 9:10] / (8.0 * cells), (8, 128))
    inv = 1.0 / nu
    sig1, inv1 = sigma[0:1], inv[0:1]
    for y in range(ly):
        p1[y] = (vp[1, 1 + y] - sig1 * vp[0, 1 + y]) * inv1
    ar_start(1, gram(1))

    for y in order:
        image = x_terms(1, y, local_terms(1, y))
        vp[2, 1 + y] = ((image - sig1 * vp[1, 1 + y]) * inv1 - sig1 * p1[y]) * inv1
        send_row(2, y)
    ar_start(2, gram(2))

    for y in order:
        image = x_terms(2, y, local_terms(2, y))
        p3[y] = (image - sig1 * vp[2, 1 + y]) * inv1
    ar_start(3, gram(3))

    weights, factors = [], []
    empty = jnp.zeros((8, 128), F32)

    def pad_rows(pieces):
        return jnp.concatenate(pieces + [empty] * (16 - len(pieces)), axis=0)

    def factor(n, red):
        base = 8 * n
        unit = jnp.where(lane == base + row, 1.0, 0.0).astype(F32)
        d = jnp.where(lane < base + 8, red, 0.0)
        shifted = pltpu.roll(d, 128 - base, 1) if n else d
        if n:
            rt = dot_nt(d, pad_rows(weights))
            s = shifted - dot_nt(rt, pad_rows([rt]))
            aug = unit - rt
        else:
            rt = empty
            s = shifted
            aug = unit
        cols = [jnp.broadcast_to(s[:, c:c + 1], (8, 128)) for c in range(8)]
        low = rt
        for k in range(8):
            piv = jnp.broadcast_to(cols[k][k:k + 1], (8, 128))
            rs = lax.rsqrt(piv)
            rs = rs * (1.5 - 0.5 * piv * rs * rs)
            lk = jnp.where(row >= k, cols[k] * rs, 0.0)
            low = low + jnp.where(lane == base + k, lk, 0.0)
            arow = jnp.broadcast_to(aug[k:k + 1], (8, 128)) * rs
            aug = jnp.where(row == k, arow, aug - jnp.where(row > k, lk, 0.0) * arow)
            for c in range(k + 1, 8):
                cols[c] = cols[c] - lk * jnp.broadcast_to(lk[c:c + 1], (8, 128))
        weights.append(dot_nn(aug, pad_rows(weights + [unit])) if n else aug)
        factors.append(low)

    def emit(n):
        q = dot_nn(weights[n][:, :8 * (n + 1)], stack(n + 1))
        for y in range(ly):
            for a in range(nb):
                c = (y * nb + a) * 128
                ob[n, pl.ds(a * nr * ly + y, 8, stride=ly), :] = q[:, c:c + 128]
        pltpu.make_async_copy(ob.at[n], basis_hbm.at[n], out_sem.at[n]).start()

    factor(0, red0)
    emit(0)
    factor(1, ar_done(1))
    emit(1)
    factor(2, ar_done(2))
    emit(2)
    factor(3, ar_done(3))
    emit(3)
    h = dot_nn(jnp.concatenate(weights[:3] + [empty], axis=0), pad_rows(factors[1:]))
    hr = lax.broadcasted_iota(jnp.int32, (32, 128), 0)
    hl = lax.broadcasted_iota(jnp.int32, (32, 128), 1)
    hess_ref[...] = h * nu[0:1] + jnp.where(hr == hl, sigma[0:1], 0.0)

    for n in range(ITERS):
        for y in range(ly):
            for side, entry in enumerate(x_sides):
                when(entry[1], lambda: x_copy(n, side, y).wait_send())
            for side in range(2):
                pl.when(z_to[side])(lambda: z_copy(n, side, y).wait_send())
        for side in range(2):
            pl.when(y_to[side])(lambda: y_copy(n, side).wait_send())
    for m in range(4):
        pltpu.make_async_copy(ab.at[m, 0:ndev - 1], ab.at[m, 0:ndev - 1], a_send.at[m]).wait()
        pltpu.make_async_copy(ob.at[m], basis_hbm.at[m], out_sem.at[m]).wait()


def shards(mesh_sizes, rhs, blocks):
    nb, nr, lx, ly, lz = rhs.shape
    assert nb == 8 and nr == 8 and lx == 1 and lz == 128
    nx, ny, nz = mesh_sizes
    ndev = nx * ny * nz
    sides = max(1, min(2, nx - 1))
    rhs2 = rhs.reshape(nb * nr * ly, lz)
    blk2 = blocks.reshape(7, nb, nb * ly, lz)
    dma = pltpu.SemaphoreType.DMA
    vm = lambda *s: pltpu.VMEM(s, F32)
    basis, hess = pl.pallas_call(
        functools.partial(kernel, mesh_sizes, nb, nr, ly, lz),
        out_shape=(
            jax.ShapeDtypeStruct((ITERS + 1, nb * nr * ly, lz), F32),
            jax.ShapeDtypeStruct((32, 128), F32),
        ),
        in_specs=[pl.BlockSpec(memory_space=pl.ANY)] * 2,
        out_specs=(pl.BlockSpec(memory_space=pl.ANY), pl.BlockSpec(memory_space=pltpu.VMEM)),
        scratch_shapes=[
            vm(nb * nr * ly, lz),
            pltpu.VMEM((7, nb, nb * ly, lz), jnp.bfloat16),
            vm(ITERS, ly + 2, nb * 8, lz),
            vm(ly, nb * 8, lz),
            vm(ly, nb * 8, lz),
            vm(ITERS, sides, ly, nb * 8, lz),
            vm(ITERS, 2, ly, 8, lz),
            vm(ITERS, 2, ly, 8, lz),
            vm(5 + sides, ly, nb, nb * 8, lz),
            vm(2, nb * 8, lz),
            vm(ITERS + 1, ndev, 2, lz),
            vm(ITERS + 1, nb * nr * ly, lz),
            dma((ITERS, sides, ly)), dma((ITERS, sides, ly)),
            dma((ITERS, 2)), dma((ITERS, 2)),
            dma((ITERS, 2, ly)), dma((ITERS, 2, ly)),
            dma((ITERS + 1,)), dma((ITERS + 1,)),
            dma((2,)), dma((ITERS + 1,)),
        ],
        compiler_params=pltpu.CompilerParams(has_side_effects=True, vmem_limit_bytes=48 * 1024 * 1024),
    )(rhs2, blk2)
    basis = basis.reshape(ITERS + 1, nb, nr, lx, ly, lz)
    hess = hess[:24, :32].reshape(3, 8, 4, 8).transpose(2, 3, 0, 1)
    return basis, hess


def solution(mesh):
    sizes = tuple(mesh.shape[a] for a in AXES)
    return jax.shard_map(
        functools.partial(shards, sizes),
        mesh=mesh,
        in_specs=(P(None, None, "gx", "gy", "gz"), P(None, None, None, "gx", "gy", "gz")),
        out_specs=(P(None, None, None, "gx", "gy", "gz"), P()),
        check_vma=False,
    )
```

```python
import functools

import jax
import jax.numpy as jnp
from jax import lax
from jax.experimental import pallas as pl
from jax.experimental.pallas import tpu as pltpu
from jax.sharding import PartitionSpec as P

ITERS = 3
F32 = jnp.float32
HIGH = lax.Precision.HIGHEST
AXES = ("gx", "gy", "gz")


def dot_nt(a, b):
    return lax.dot_general(a, b, (((1,), (1,)), ((), ())), precision=HIGH, preferred_element_type=F32)


def dot_nn(a, b):
    return lax.dot_general(a, b, (((1,), (0,)), ((), ())), precision=HIGH, preferred_element_type=F32)


def kernel(
    mesh_sizes, nb, nr, ly, lz,
    rhs_hbm, blk_hbm, basis_hbm, hess_ref,
    rv, bv, vp, p1, p3, xb, zs, zr, ce, zp, ab, ob,
    x_send, x_recv, y_send, y_recv, z_send, z_recv, a_send, a_recv, in_sem, out_sem,
):
    nx, ny, nz = mesh_sizes
    ndev = nx * ny * nz
    gx, gy, gz = (lax.axis_index(a) for a in AXES)
    me = (gx * ny + gy) * nz + gz
    cells = ndev * ly * lz

    row = lax.broadcasted_iota(jnp.int32, (8, 128), 0)
    lane = lax.broadcasted_iota(jnp.int32, (8, 128), 1)

    def peer(d):
        t = lax.rem(me + d, ndev)
        return (t // (ny * nz), (t // nz) % ny, t % nz)

    barrier = pltpu.get_barrier_semaphore()

    def greet(d, c):
        pl.semaphore_signal(barrier, inc=1, device_id=peer(d), device_id_type=pl.DeviceIdType.MESH)
        return c

    in_rhs = pltpu.make_async_copy(rhs_hbm, rv, in_sem.at[0])
    in_blk = pltpu.make_async_copy(blk_hbm, bv, in_sem.at[1])
    in_rhs.start()
    in_blk.start()
    lax.fori_loop(1, ndev, greet, 0)

    if nx == 1:
        x_sides = []
    elif nx == 2:
        x_sides = [(1 + gx, None, 1 - gx)]
    else:
        x_sides = [(1, gx < nx - 1, gx + 1), (2, gx > 0, gx - 1)]

    def when(cond, fn):
        if cond is None:
            fn()
        else:
            pl.when(cond)(fn)

    def remote(src, dst, ssem, rsem, dev):
        return pltpu.make_async_remote_copy(
            src_ref=src, dst_ref=dst, send_sem=ssem, recv_sem=rsem,
            device_id=dev, device_id_type=pl.DeviceIdType.MESH,
        )

    def x_copy(n, side, y):
        opposite = side if nx == 2 else 1 - side
        return remote(vp.at[n, 1 + y], xb.at[n, opposite, y], x_send.at[n, side, y],
                      x_recv.at[n, opposite, y], {"gx": x_sides[side][2]})

    def x_arrived(n, side, y):
        remote(vp.at[n, 1 + y], xb.at[n, side, y], x_send.at[n, side, y],
               x_recv.at[n, side, y], {"gx": x_sides[side][2]}).wait_recv()

    def y_copy(n, side):
        if side == 0:
            return remote(vp.at[n, ly], vp.at[n, 0], y_send.at[n, 0], y_recv.at[n, 0], {"gy": gy + 1})
        return remote(vp.at[n, 1], vp.at[n, ly + 1], y_send.at[n, 1], y_recv.at[n, 1], {"gy": gy - 1})

    def z_copy(n, side, y):
        target = gz - 1 if side == 0 else gz + 1
        return remote(zs.at[n, side, y], zr.at[n, side, y], z_send.at[n, side, y],
                      z_recv.at[n, side, y], {"gz": target})

    y_to = (gy < ny - 1, gy > 0)
    y_from = (gy > 0, gy < ny - 1)
    z_to = (gz > 0, gz < nz - 1)
    z_from = (gz < nz - 1, gz > 0)

    for side in range(2):
        @pl.when(jnp.logical_not(y_from[side]))
        def _():
            for n in range(ITERS):
                vp[n, 0 if side == 0 else ly + 1] = jnp.zeros((nb * 8, 128), F32)

        @pl.when(jnp.logical_not(z_from[side]))
        def _():
            for n in range(ITERS):
                zr[n, side] = jnp.zeros((ly, 8, 128), F32)

    if nx > 2:
        for side in range(2):
            @pl.when(jnp.logical_not(x_sides[side][1]))
            def _():
                for n in range(ITERS):
                    xb[n, side] = jnp.zeros((ly, nb * 8, 128), F32)

    def send_row(n, y):
        for side, entry in enumerate(x_sides):
            when(entry[1], lambda: x_copy(n, side, y).start())
        first = jnp.zeros((8, 128), F32)
        last = jnp.zeros((8, 128), F32)
        for a in range(nb):
            v = vp[n, 1 + y, a * 8:(a + 1) * 8]
            first = jnp.where(lane == a, pltpu.roll(v, a, 1) if a else v, first)
            last = jnp.where(lane == a, pltpu.roll(v, a + 1, 1), last)
        zs[n, 0, y] = first
        zs[n, 1, y] = last
        for side in range(2):
            pl.when(z_to[side])(lambda: z_copy(n, side, y).start())
        if y == ly - 1:
            pl.when(y_to[0])(lambda: y_copy(n, 0).start())
        if y == 0:
            pl.when(y_to[1])(lambda: y_copy(n, 1).start())

    order = [0] + ([ly - 1] if ly > 1 else []) + list(range(1, ly - 1))

    in_rhs.wait()
    for y in order:
        for a in range(nb):
            vp[0, 1 + y, a * 8:(a + 1) * 8] = rv[pl.ds(a * nr * ly + y, 8, stride=ly), :]
    pl.semaphore_wait(barrier, ndev - 1)
    for y in order:
        send_row(0, y)

    in_blk.wait()
    terms = [0, 3, 4, 5, 6] + [e[0] for e in x_sides]
    total_abs = jnp.zeros((8, 128), F32)
    for t, k in enumerate(terms):
        def expand(i, carry):
            rows = bv[k, i].astype(F32)
            for j in range(nb):
                for y in range(ly):
                    r = j * ly + y
                    wide = jnp.broadcast_to(rows[r:r + 1], (8, 128))
                    ce[t, y, j, pl.ds(pl.multiple_of(i * 8, 8), 8), :] = wide
                    if j == 0 and y == 0:
                        pass
            return carry + jnp.sum(jnp.abs(rows), axis=0, keepdims=True)
        total_abs = lax.fori_loop(0, nb, expand, total_abs)
    trace = jnp.zeros((8, 128), F32)
    for y in range(ly):
        for i in range(nb):
            trace = trace + ce[0, y, i, i * 8:(i + 1) * 8]

    def wide(field):
        return jnp.concatenate(
            [field(y, a) for y in range(ly) for a in range(nb)], axis=1)

    def eight(a):
        return a * 8 if isinstance(a, int) else pl.multiple_of(a * 8, 8)

    def blockview(ref, n, off):
        if n is None:
            return lambda y, a: ref[y, pl.ds(eight(a), 8), :]
        return lambda y, a: ref[n, off + y, pl.ds(eight(a), 8), :]

    views = [blockview(vp, 0, 1), blockview(p1, None, 0), blockview(vp, 2, 1), blockview(p3, None, 0)]

    def stack(count):
        return jnp.concatenate([wide(v) for v in views[:count]], axis=0)

    def gram_row(n, y, acc):
        def body(a, acc):
            p = views[n](y, a)
            parts = []
            for i in range(n + 1):
                q = views[i](y, a)
                for d in range(8):
                    parts.append(acc[i * 8 + d] + p * (pltpu.roll(q, 8 - d, 0) if d else q))
            return tuple(parts)
        return lax.fori_loop(0, nb, body, acc)

    def gram_zero(n):
        return tuple(jnp.zeros((8, 128), F32) for _ in range(8 * (n + 1)))

    def gram_end(acc):
        d8 = jnp.zeros((8, 128), F32)
        for k, part in enumerate(acc):
            where = lane % 32 == (k // 8) * 8 + (row + k % 8) % 8
            d8 = jnp.where(where, jnp.sum(part, axis=1, keepdims=True), d8)
        return d8

    def gram(n):
        acc = gram_zero(n)
        for y in range(ly):
            acc = gram_row(n, y, acc)
        return gram_end(acc)

    def ar_start(m, d8):
        packed = jnp.where(lane // 32 == row % 4, d8, 0.0)
        ab[m, me, 0:1] = jnp.sum(packed[0:4], axis=0, keepdims=True)
        ab[m, me, 1:2] = jnp.sum(packed[4:8], axis=0, keepdims=True)

        def body(d, c):
            remote(ab.at[m, me], ab.at[m, me], a_send.at[m], a_recv.at[m], peer(d)).start()
            return c
        lax.fori_loop(1, ndev, body, 0)

    def ar_done(m):
        pltpu.make_async_copy(ab.at[m, 0:ndev - 1], ab.at[m, 0:ndev - 1], a_recv.at[m]).wait()
        total = jnp.sum(ab[m], axis=0)
        z = jnp.where(row < 4, total[0:1], total[1:2])
        z = jnp.where(lane // 32 == row % 4, z, 0.0)
        z = z + pltpu.roll(z, 64, 1)
        return z + pltpu.roll(z, 32, 1)

    lane_sum = lambda x: jnp.sum(x, axis=1, keepdims=True)
    d0 = gram(0)
    d0 = d0 + jnp.where(lane % 32 == 8, lane_sum(trace), 0.0)
    d0 = d0 + jnp.where(lane % 32 == 9, lane_sum(total_abs), 0.0)
    ar_start(0, d0)

    def local_terms(n, y):
        pl_z = [z_from[0], z_from[1]]
        for side in range(2):
            pl.when(pl_z[side])(lambda: z_copy(n, side, y).wait_recv())
        if y == 0:
            pl.when(y_from[0])(lambda: y_copy(n, 0).wait_recv())
        if y == ly - 1:
            pl.when(y_from[1])(lambda: y_copy(n, 1).wait_recv())
        plus, minus = zr[n, 0, y], zr[n, 1, y]
        for j in range(nb):
            v = vp[n, 1 + y, j * 8:(j + 1) * 8]
            zp[0, j * 8:(j + 1) * 8] = jnp.where(
                lane == lz - 1, pltpu.roll(plus, lz - 1 - j, 1), pltpu.roll(v, lz - 1, 1))
            zp[1, j * 8:(j + 1) * 8] = jnp.where(
                lane == 0, pltpu.roll(minus, lz - j, 1) if j else minus, pltpu.roll(v, 1, 1))

        def body(j, acc):
            at = pl.ds(pl.multiple_of(j * 8, 8), 8)
            values = [vp[n, 1 + y, at, :], vp[n, 2 + y, at, :], vp[n, y, at, :], zp[0, at, :], zp[1, at, :]]
            for t, v in enumerate(values):
                acc = acc + ce[t, y, j].reshape(nb, 8, 128) * v[None]
            return acc
        return lax.fori_loop(0, nb, body, jnp.zeros((nb, 8, 128), F32))

    def x_terms(n, y, acc):
        for side, entry in enumerate(x_sides):
            when(entry[1], lambda: x_arrived(n, side, y))

            def body(j, acc):
                at = pl.ds(pl.multiple_of(j * 8, 8), 8)
                return acc + ce[5 + side, y, j].reshape(nb, 8, 128) * xb[n, side, y, at, :][None]
            acc = lax.fori_loop(0, nb, body, acc)
        return acc.reshape(nb * 8, 128)

    weights, factors = [], []
    empty = jnp.zeros((8, 128), F32)

    def pad_rows(pieces):
        return jnp.concatenate(pieces + [empty] * (16 - len(pieces)), axis=0)

    def factor(n, red):
        base = 8 * n
        unit = jnp.where(lane == base + row, 1.0, 0.0).astype(F32)
        d = jnp.where(lane < base + 8, red, 0.0)
        shifted = pltpu.roll(d, 128 - base, 1) if n else d
        if n:
            rt = dot_nt(d, pad_rows(weights))
            s = shifted - dot_nt(rt, pad_rows([rt]))
            aug = unit - rt
        else:
            rt = empty
            s = shifted
            aug = unit
        cols = [jnp.broadcast_to(s[:, c:c + 1], (8, 128)) for c in range(8)]
        low = rt
        for k in range(8):
            piv = jnp.broadcast_to(cols[k][k:k + 1], (8, 128))
            rs = lax.rsqrt(piv)
            rs = rs * (1.5 - 0.5 * piv * rs * rs)
            lk = jnp.where(row >= k, cols[k] * rs, 0.0)
            low = low + jnp.where(lane == base + k, lk, 0.0)
            arow = jnp.broadcast_to(aug[k:k + 1], (8, 128)) * rs
            aug = jnp.where(row == k, arow, aug - jnp.where(row > k, lk, 0.0) * arow)
            for c in range(k + 1, 8):
                cols[c] = cols[c] - lk * jnp.broadcast_to(lk[c:c + 1], (8, 128))
        weights.append(dot_nn(aug, pad_rows(weights + [unit])) if n else aug)
        factors.append(low)

    def emit(n):
        q = dot_nn(weights[n][:, :8 * (n + 1)], stack(n + 1))
        for y in range(ly):
            for a in range(nb):
                c = (y * nb + a) * 128
                ob[n, pl.ds(a * nr * ly + y, 8, stride=ly), :] = q[:, c:c + 128]
        pltpu.make_async_copy(ob.at[n], basis_hbm.at[n], out_sem.at[n]).start()

    for y in order:
        vp[1, 1 + y] = x_terms(0, y, local_terms(0, y))
        send_row(1, y)
    red0 = ar_done(0)
    sigma = jnp.broadcast_to(red0[0:1, 8:9] / (8.0 * cells), (8, 128))
    nu = jnp.broadcast_to(red0[0:1, 9:10] / (8.0 * cells), (8, 128))
    inv = 1.0 / nu
    sig1, inv1 = sigma[0:1], inv[0:1]
    for y in range(ly):
        p1[y] = (vp[1, 1 + y] - sig1 * vp[0, 1 + y]) * inv1
    ar_start(1, gram(1))
    factor(0, red0)
    emit(0)

    acc = gram_zero(2)
    for y in order:
        image = x_terms(1, y, local_terms(1, y))
        vp[2, 1 + y] = ((image - sig1 * vp[1, 1 + y]) * inv1 - sig1 * p1[y]) * inv1
        send_row(2, y)
        acc = gram_row(2, y, acc)
    ar_start(2, gram_end(acc))

    acc = gram_zero(3)
    for y in order:
        image = x_terms(2, y, local_terms(2, y))
        p3[y] = (image - sig1 * vp[2, 1 + y]) * inv1
        acc = gram_row(3, y, acc)
    ar_start(3, gram_end(acc))

    factor(1, ar_done(1))
    emit(1)
    factor(2, ar_done(2))
    emit(2)
    factor(3, ar_done(3))
    emit(3)
    h = dot_nn(jnp.concatenate(weights[:3] + [empty], axis=0), pad_rows(factors[1:]))
    hr = lax.broadcasted_iota(jnp.int32, (32, 128), 0)
    hl = lax.broadcasted_iota(jnp.int32, (32, 128), 1)
    hess_ref[...] = h * nu[0:1] + jnp.where(hr == hl, sigma[0:1], 0.0)

    for n in range(ITERS):
        for y in range(ly):
            for side, entry in enumerate(x_sides):
                when(entry[1], lambda: x_copy(n, side, y).wait_send())
            for side in range(2):
                pl.when(z_to[side])(lambda: z_copy(n, side, y).wait_send())
        for side in range(2):
            pl.when(y_to[side])(lambda: y_copy(n, side).wait_send())
    for m in range(4):
        pltpu.make_async_copy(ab.at[m, 0:ndev - 1], ab.at[m, 0:ndev - 1], a_send.at[m]).wait()
        pltpu.make_async_copy(ob.at[m], basis_hbm.at[m], out_sem.at[m]).wait()


def shards(mesh_sizes, rhs, blocks):
    nb, nr, lx, ly, lz = rhs.shape
    assert nb == 8 and nr == 8 and lx == 1 and lz == 128
    nx, ny, nz = mesh_sizes
    ndev = nx * ny * nz
    sides = max(1, min(2, nx - 1))
    rhs2 = rhs.reshape(nb * nr * ly, lz)
    blk2 = blocks.reshape(7, nb, nb * ly, lz)
    dma = pltpu.SemaphoreType.DMA
    vm = lambda *s: pltpu.VMEM(s, F32)
    basis, hess = pl.pallas_call(
        functools.partial(kernel, mesh_sizes, nb, nr, ly, lz),
        out_shape=(
            jax.ShapeDtypeStruct((ITERS + 1, nb * nr * ly, lz), F32),
            jax.ShapeDtypeStruct((32, 128), F32),
        ),
        in_specs=[pl.BlockSpec(memory_space=pl.ANY)] * 2,
        out_specs=(pl.BlockSpec(memory_space=pl.ANY), pl.BlockSpec(memory_space=pltpu.VMEM)),
        scratch_shapes=[
            vm(nb * nr * ly, lz),
            pltpu.VMEM((7, nb, nb * ly, lz), jnp.bfloat16),
            vm(ITERS, ly + 2, nb * 8, lz),
            vm(ly, nb * 8, lz),
            vm(ly, nb * 8, lz),
            vm(ITERS, sides, ly, nb * 8, lz),
            vm(ITERS, 2, ly, 8, lz),
            vm(ITERS, 2, ly, 8, lz),
            vm(5 + sides, ly, nb, nb * 8, lz),
            vm(2, nb * 8, lz),
            vm(ITERS + 1, ndev, 2, lz),
            vm(ITERS + 1, nb * nr * ly, lz),
            dma((ITERS, sides, ly)), dma((ITERS, sides, ly)),
            dma((ITERS, 2)), dma((ITERS, 2)),
            dma((ITERS, 2, ly)), dma((ITERS, 2, ly)),
            dma((ITERS + 1,)), dma((ITERS + 1,)),
            dma((2,)), dma((ITERS + 1,)),
        ],
        compiler_params=pltpu.CompilerParams(collective_id=0, has_side_effects=True, vmem_limit_bytes=48 * 1024 * 1024),
    )(rhs2, blk2)
    basis = basis.reshape(ITERS + 1, nb, nr, lx, ly, lz)
    hess = hess[:24, :32].reshape(3, 8, 4, 8).transpose(2, 3, 0, 1)
    return basis, hess


def solution(mesh):
    sizes = tuple(mesh.shape[a] for a in AXES)
    return jax.shard_map(
        functools.partial(shards, sizes),
        mesh=mesh,
        in_specs=(P(None, None, "gx", "gy", "gz"), P(None, None, None, "gx", "gy", "gz")),
        out_specs=(P(None, None, None, "gx", "gy", "gz"), P()),
        check_vma=False,
    )
```

```python
import functools

import jax
import jax.numpy as jnp
from jax import lax
from jax.experimental import pallas as pl
from jax.experimental.pallas import tpu as pltpu
from jax.sharding import PartitionSpec as P

ITERS = 3
F32 = jnp.float32
HIGH = lax.Precision.HIGHEST
AXES = ("gx", "gy", "gz")


def dot_nt(a, b):
    return lax.dot_general(a, b, (((1,), (1,)), ((), ())), precision=HIGH, preferred_element_type=F32)


def dot_nn(a, b):
    return lax.dot_general(a, b, (((1,), (0,)), ((), ())), precision=HIGH, preferred_element_type=F32)


def kernel(
    mesh_sizes, nb, nr, ly, lz,
    rhs_hbm, blk_hbm, basis_hbm, hess_ref,
    rv, bv, vp, p1, p3, xb, zs, zr, ce, zp, ab, ob,
    x_send, x_recv, y_send, y_recv, z_send, z_recv, a_send, a_recv, in_sem, out_sem, known,
):
    nx, ny, nz = mesh_sizes
    ndev = nx * ny * nz
    gx, gy, gz = (lax.axis_index(a) for a in AXES)
    me = (gx * ny + gy) * nz + gz
    cells = ndev * ly * lz

    row = lax.broadcasted_iota(jnp.int32, (8, 128), 0)
    lane = lax.broadcasted_iota(jnp.int32, (8, 128), 1)

    def peer(d):
        t = lax.rem(me + d, ndev)
        return (t // (ny * nz), (t // nz) % ny, t % nz)

    barrier = pltpu.get_barrier_semaphore()

    def greet(sem, axis):
        size, at = {"gx": (nx, gx), "gy": (ny, gy), "gz": (nz, gz)}[axis]

        def body(d, c):
            pl.semaphore_signal(sem, inc=1, device_id={axis: lax.rem(at + d, size)},
                                device_id_type=pl.DeviceIdType.MESH)
            return c
        lax.fori_loop(1, size, body, 0)

    in_rhs = pltpu.make_async_copy(rhs_hbm, rv, in_sem.at[0])
    in_blk = pltpu.make_async_copy(blk_hbm, bv, in_sem.at[1])
    in_rhs.start()
    in_blk.start()
    for axis in AXES:
        greet(barrier, axis)

    if nx == 1:
        x_sides = []
    elif nx == 2:
        x_sides = [(1 + gx, None, 1 - gx)]
    else:
        x_sides = [(1, gx < nx - 1, gx + 1), (2, gx > 0, gx - 1)]

    def when(cond, fn):
        if cond is None:
            fn()
        else:
            pl.when(cond)(fn)

    def remote(src, dst, ssem, rsem, dev):
        return pltpu.make_async_remote_copy(
            src_ref=src, dst_ref=dst, send_sem=ssem, recv_sem=rsem,
            device_id=dev, device_id_type=pl.DeviceIdType.MESH,
        )

    def x_copy(n, side, y):
        opposite = side if nx == 2 else 1 - side
        return remote(vp.at[n, 1 + y], xb.at[n, opposite, y], x_send.at[n, side, y],
                      x_recv.at[n, opposite, y], {"gx": x_sides[side][2]})

    def x_arrived(n, side, y):
        remote(vp.at[n, 1 + y], xb.at[n, side, y], x_send.at[n, side, y],
               x_recv.at[n, side, y], {"gx": x_sides[side][2]}).wait_recv()

    def y_copy(n, side):
        if side == 0:
            return remote(vp.at[n, ly], vp.at[n, 0], y_send.at[n, 0], y_recv.at[n, 0], {"gy": gy + 1})
        return remote(vp.at[n, 1], vp.at[n, ly + 1], y_send.at[n, 1], y_recv.at[n, 1], {"gy": gy - 1})

    def z_copy(n, side, y):
        target = gz - 1 if side == 0 else gz + 1
        return remote(zs.at[n, side, y], zr.at[n, side, y], z_send.at[n, side, y],
                      z_recv.at[n, side, y], {"gz": target})

    y_to = (gy < ny - 1, gy > 0)
    y_from = (gy > 0, gy < ny - 1)
    z_to = (gz > 0, gz < nz - 1)
    z_from = (gz < nz - 1, gz > 0)

    for side in range(2):
        @pl.when(jnp.logical_not(y_from[side]))
        def _():
            for n in range(ITERS):
                vp[n, 0 if side == 0 else ly + 1] = jnp.zeros((nb * 8, 128), F32)

        @pl.when(jnp.logical_not(z_from[side]))
        def _():
            for n in range(ITERS):
                zr[n, side] = jnp.zeros((ly, 8, 128), F32)

    if nx > 2:
        for side in range(2):
            @pl.when(jnp.logical_not(x_sides[side][1]))
            def _():
                for n in range(ITERS):
                    xb[n, side] = jnp.zeros((ly, nb * 8, 128), F32)

    def send_row(n, y):
        for side, entry in enumerate(x_sides):
            when(entry[1], lambda: x_copy(n, side, y).start())
        first = jnp.zeros((8, 128), F32)
        last = jnp.zeros((8, 128), F32)
        for a in range(nb):
            v = vp[n, 1 + y, a * 8:(a + 1) * 8]
            first = jnp.where(lane == a, pltpu.roll(v, a, 1) if a else v, first)
            last = jnp.where(lane == a, pltpu.roll(v, a + 1, 1), last)
        zs[n, 0, y] = first
        zs[n, 1, y] = last
        for side in range(2):
            pl.when(z_to[side])(lambda: z_copy(n, side, y).start())
        if y == ly - 1:
            pl.when(y_to[0])(lambda: y_copy(n, 0).start())
        if y == 0:
            pl.when(y_to[1])(lambda: y_copy(n, 1).start())

    order = [0] + ([ly - 1] if ly > 1 else []) + list(range(1, ly - 1))

    in_rhs.wait()
    for y in order:
        for a in range(nb):
            vp[0, 1 + y, a * 8:(a + 1) * 8] = rv[pl.ds(a * nr * ly + y, 8, stride=ly), :]
    pl.semaphore_wait(barrier, nx + ny + nz - 3)
    greet(known.at[0], "gy")
    for y in order:
        send_row(0, y)
    pl.semaphore_wait(known.at[0], ny - 1)
    greet(known.at[1], "gx")

    in_blk.wait()
    terms = [0, 3, 4, 5, 6] + [e[0] for e in x_sides]
    total_abs = jnp.zeros((8, 128), F32)
    for t, k in enumerate(terms):
        def expand(i, carry):
            rows = bv[k, i].astype(F32)
            for j in range(nb):
                for y in range(ly):
                    r = j * ly + y
                    wide = jnp.broadcast_to(rows[r:r + 1], (8, 128))
                    ce[t, y, j, pl.ds(pl.multiple_of(i * 8, 8), 8), :] = wide
                    if j == 0 and y == 0:
                        pass
            return carry + jnp.sum(jnp.abs(rows), axis=0, keepdims=True)
        total_abs = lax.fori_loop(0, nb, expand, total_abs)
    trace = jnp.zeros((8, 128), F32)
    for y in range(ly):
        for i in range(nb):
            trace = trace + ce[0, y, i, i * 8:(i + 1) * 8]

    def wide(field):
        return jnp.concatenate(
            [field(y, a) for y in range(ly) for a in range(nb)], axis=1)

    def eight(a):
        return a * 8 if isinstance(a, int) else pl.multiple_of(a * 8, 8)

    def blockview(ref, n, off):
        if n is None:
            return lambda y, a: ref[y, pl.ds(eight(a), 8), :]
        return lambda y, a: ref[n, off + y, pl.ds(eight(a), 8), :]

    views = [blockview(vp, 0, 1), blockview(p1, None, 0), blockview(vp, 2, 1), blockview(p3, None, 0)]

    def stack(count):
        return jnp.concatenate([wide(v) for v in views[:count]], axis=0)

    def gram_row(n, y, acc):
        def body(a, acc):
            p = views[n](y, a)
            parts = []
            for i in range(n + 1):
                q = views[i](y, a)
                for d in range(8):
                    parts.append(acc[i * 8 + d] + p * (pltpu.roll(q, 8 - d, 0) if d else q))
            return tuple(parts)
        return lax.fori_loop(0, nb, body, acc)

    def gram_zero(n):
        return tuple(jnp.zeros((8, 128), F32) for _ in range(8 * (n + 1)))

    def gram_end(acc):
        d8 = jnp.zeros((8, 128), F32)
        for k, part in enumerate(acc):
            where = lane % 32 == (k // 8) * 8 + (row + k % 8) % 8
            d8 = jnp.where(where, jnp.sum(part, axis=1, keepdims=True), d8)
        return d8

    def gram(n):
        acc = gram_zero(n)
        for y in range(ly):
            acc = gram_row(n, y, acc)
        return gram_end(acc)

    def ar_start(m, d8):
        packed = jnp.where(lane // 32 == row % 4, d8, 0.0)
        ab[m, me, 0:1] = jnp.sum(packed[0:4], axis=0, keepdims=True)
        ab[m, me, 1:2] = jnp.sum(packed[4:8], axis=0, keepdims=True)

        def body(d, c):
            remote(ab.at[m, me], ab.at[m, me], a_send.at[m], a_recv.at[m], peer(d)).start()
            return c
        lax.fori_loop(1, ndev, body, 0)

    def ar_done(m):
        pltpu.make_async_copy(ab.at[m, 0:ndev - 1], ab.at[m, 0:ndev - 1], a_recv.at[m]).wait()
        total = jnp.sum(ab[m], axis=0)
        z = jnp.where(row < 4, total[0:1], total[1:2])
        z = jnp.where(lane // 32 == row % 4, z, 0.0)
        z = z + pltpu.roll(z, 64, 1)
        return z + pltpu.roll(z, 32, 1)

    lane_sum = lambda x: jnp.sum(x, axis=1, keepdims=True)
    d0 = gram(0)
    d0 = d0 + jnp.where(lane % 32 == 8, lane_sum(trace), 0.0)
    d0 = d0 + jnp.where(lane % 32 == 9, lane_sum(total_abs), 0.0)
    pl.semaphore_wait(known.at[1], nx - 1)
    ar_start(0, d0)

    def local_terms(n, y):
        pl_z = [z_from[0], z_from[1]]
        for side in range(2):
            pl.when(pl_z[side])(lambda: z_copy(n, side, y).wait_recv())
        if y == 0:
            pl.when(y_from[0])(lambda: y_copy(n, 0).wait_recv())
        if y == ly - 1:
            pl.when(y_from[1])(lambda: y_copy(n, 1).wait_recv())
        plus, minus = zr[n, 0, y], zr[n, 1, y]
        for j in range(nb):
            v = vp[n, 1 + y, j * 8:(j + 1) * 8]
            zp[0, j * 8:(j + 1) * 8] = jnp.where(
                lane == lz - 1, pltpu.roll(plus, lz - 1 - j, 1), pltpu.roll(v, lz - 1, 1))
            zp[1, j * 8:(j + 1) * 8] = jnp.where(
                lane == 0, pltpu.roll(minus, lz - j, 1) if j else minus, pltpu.roll(v, 1, 1))

        def body(j, acc):
            at = pl.ds(pl.multiple_of(j * 8, 8), 8)
            values = [vp[n, 1 + y, at, :], vp[n, 2 + y, at, :], vp[n, y, at, :], zp[0, at, :], zp[1, at, :]]
            for t, v in enumerate(values):
                acc = acc + ce[t, y, j].reshape(nb, 8, 128) * v[None]
            return acc
        return lax.fori_loop(0, nb, body, jnp.zeros((nb, 8, 128), F32))

    def x_terms(n, y, acc):
        for side, entry in enumerate(x_sides):
            when(entry[1], lambda: x_arrived(n, side, y))

            def body(j, acc):
                at = pl.ds(pl.multiple_of(j * 8, 8), 8)
                return acc + ce[5 + side, y, j].reshape(nb, 8, 128) * xb[n, side, y, at, :][None]
            acc = lax.fori_loop(0, nb, body, acc)
        return acc.reshape(nb * 8, 128)

    weights, factors = [], []
    empty = jnp.zeros((8, 128), F32)

    def pad_rows(pieces):
        return jnp.concatenate(pieces + [empty] * (16 - len(pieces)), axis=0)

    def factor(n, red):
        base = 8 * n
        unit = jnp.where(lane == base + row, 1.0, 0.0).astype(F32)
        d = jnp.where(lane < base + 8, red, 0.0)
        shifted = pltpu.roll(d, 128 - base, 1) if n else d
        if n:
            rt = dot_nt(d, pad_rows(weights))
            s = shifted - dot_nt(rt, pad_rows([rt]))
            aug = unit - rt
        else:
            rt = empty
            s = shifted
            aug = unit
        cols = [jnp.broadcast_to(s[:, c:c + 1], (8, 128)) for c in range(8)]
        low = rt
        for k in range(8):
            piv = jnp.broadcast_to(cols[k][k:k + 1], (8, 128))
            rs = lax.rsqrt(piv)
            rs = rs * (1.5 - 0.5 * piv * rs * rs)
            lk = jnp.where(row >= k, cols[k] * rs, 0.0)
            low = low + jnp.where(lane == base + k, lk, 0.0)
            arow = jnp.broadcast_to(aug[k:k + 1], (8, 128)) * rs
            aug = jnp.where(row == k, arow, aug - jnp.where(row > k, lk, 0.0) * arow)
            for c in range(k + 1, 8):
                cols[c] = cols[c] - lk * jnp.broadcast_to(lk[c:c + 1], (8, 128))
        weights.append(dot_nn(aug, pad_rows(weights + [unit])) if n else aug)
        factors.append(low)

    def emit(n):
        q = dot_nn(weights[n][:, :8 * (n + 1)], stack(n + 1))
        for y in range(ly):
            for a in range(nb):
                c = (y * nb + a) * 128
                ob[n, pl.ds(a * nr * ly + y, 8, stride=ly), :] = q[:, c:c + 128]
        pltpu.make_async_copy(ob.at[n], basis_hbm.at[n], out_sem.at[n]).start()

    for y in order:
        vp[1, 1 + y] = x_terms(0, y, local_terms(0, y))
        send_row(1, y)
    red0 = ar_done(0)
    sigma = jnp.broadcast_to(red0[0:1, 8:9] / (8.0 * cells), (8, 128))
    nu = jnp.broadcast_to(red0[0:1, 9:10] / (8.0 * cells), (8, 128))
    inv = 1.0 / nu
    sig1, inv1 = sigma[0:1], inv[0:1]
    for y in range(ly):
        p1[y] = (vp[1, 1 + y] - sig1 * vp[0, 1 + y]) * inv1
    ar_start(1, gram(1))

    acc = gram_zero(2)
    for y in order:
        image = x_terms(1, y, local_terms(1, y))
        vp[2, 1 + y] = ((image - sig1 * vp[1, 1 + y]) * inv1 - sig1 * p1[y]) * inv1
        send_row(2, y)
        acc = gram_row(2, y, acc)
    ar_start(2, gram_end(acc))

    acc = gram_zero(3)
    for y in order:
        image = x_terms(2, y, local_terms(2, y))
        p3[y] = (image - sig1 * vp[2, 1 + y]) * inv1
        acc = gram_row(3, y, acc)
    ar_start(3, gram_end(acc))
    factor(0, red0)
    emit(0)

    factor(1, ar_done(1))
    emit(1)
    factor(2, ar_done(2))
    emit(2)
    factor(3, ar_done(3))
    emit(3)
    h = dot_nn(jnp.concatenate(weights[:3] + [empty], axis=0), pad_rows(factors[1:]))
    hr = lax.broadcasted_iota(jnp.int32, (32, 128), 0)
    hl = lax.broadcasted_iota(jnp.int32, (32, 128), 1)
    hess_ref[...] = h * nu[0:1] + jnp.where(hr == hl, sigma[0:1], 0.0)

    for n in range(ITERS):
        for y in range(ly):
            for side, entry in enumerate(x_sides):
                when(entry[1], lambda: x_copy(n, side, y).wait_send())
            for side in range(2):
                pl.when(z_to[side])(lambda: z_copy(n, side, y).wait_send())
        for side in range(2):
            pl.when(y_to[side])(lambda: y_copy(n, side).wait_send())
    for m in range(4):
        pltpu.make_async_copy(ab.at[m, 0:ndev - 1], ab.at[m, 0:ndev - 1], a_send.at[m]).wait()
        pltpu.make_async_copy(ob.at[m], basis_hbm.at[m], out_sem.at[m]).wait()


def shards(mesh_sizes, rhs, blocks):
    nb, nr, lx, ly, lz = rhs.shape
    assert nb == 8 and nr == 8 and lx == 1 and lz == 128
    nx, ny, nz = mesh_sizes
    ndev = nx * ny * nz
    sides = max(1, min(2, nx - 1))
    rhs2 = rhs.reshape(nb * nr * ly, lz)
    blk2 = blocks.reshape(7, nb, nb * ly, lz)
    dma = pltpu.SemaphoreType.DMA
    vm = lambda *s: pltpu.VMEM(s, F32)
    basis, hess = pl.pallas_call(
        functools.partial(kernel, mesh_sizes, nb, nr, ly, lz),
        out_shape=(
            jax.ShapeDtypeStruct((ITERS + 1, nb * nr * ly, lz), F32),
            jax.ShapeDtypeStruct((32, 128), F32),
        ),
        in_specs=[pl.BlockSpec(memory_space=pl.ANY)] * 2,
        out_specs=(pl.BlockSpec(memory_space=pl.ANY), pl.BlockSpec(memory_space=pltpu.VMEM)),
        scratch_shapes=[
            vm(nb * nr * ly, lz),
            pltpu.VMEM((7, nb, nb * ly, lz), jnp.bfloat16),
            vm(ITERS, ly + 2, nb * 8, lz),
            vm(ly, nb * 8, lz),
            vm(ly, nb * 8, lz),
            vm(ITERS, sides, ly, nb * 8, lz),
            vm(ITERS, 2, ly, 8, lz),
            vm(ITERS, 2, ly, 8, lz),
            vm(5 + sides, ly, nb, nb * 8, lz),
            vm(2, nb * 8, lz),
            vm(ITERS + 1, ndev, 2, lz),
            vm(ITERS + 1, nb * nr * ly, lz),
            dma((ITERS, sides, ly)), dma((ITERS, sides, ly)),
            dma((ITERS, 2)), dma((ITERS, 2)),
            dma((ITERS, 2, ly)), dma((ITERS, 2, ly)),
            dma((ITERS + 1,)), dma((ITERS + 1,)),
            dma((2,)), dma((ITERS + 1,)),
            pltpu.SemaphoreType.REGULAR((2,)),
        ],
        compiler_params=pltpu.CompilerParams(collective_id=0, has_side_effects=True, vmem_limit_bytes=48 * 1024 * 1024),
    )(rhs2, blk2)
    basis = basis.reshape(ITERS + 1, nb, nr, lx, ly, lz)
    hess = hess[:24, :32].reshape(3, 8, 4, 8).transpose(2, 3, 0, 1)
    return basis, hess


def solution(mesh):
    sizes = tuple(mesh.shape[a] for a in AXES)
    return jax.shard_map(
        functools.partial(shards, sizes),
        mesh=mesh,
        in_specs=(P(None, None, "gx", "gy", "gz"), P(None, None, None, "gx", "gy", "gz")),
        out_specs=(P(None, None, None, "gx", "gy", "gz"), P()),
        check_vma=False,
    )
```
